32 devices in a mesh: fsdp: 8 (over z, x), dp: 4 (over y, core).
Axes of the slice: x: 2, y: 2, z: 4, core: 2. Of those that a mesh axis runs over, the one named last changes fastest.
Arguments:
- features: bfloat16 [8192, 1024], P(('fsdp', 'dp')), may hold values from -6 to 6
- normed: bfloat16 [8192, 4096], P(('fsdp', 'dp')), may hold values from -6 to 6
- relu_mask: int32 [8192, 4096], P(('fsdp', 'dp')), may hold values 0 or 1
- cotangent: bfloat16 [8192, 4096], P(('fsdp', 'dp')), may hold values from -40 to 40
- weight_shard: bfloat16 [1024, 4096], P('fsdp'), may hold values from -0.1875 to 0.1875
- norm_gain: float32 [4096], replicated, may hold values from 0.25 to 1.75
- inverse_deviation: float32 [4096], replicated, may hold values from 0.5 to 3
Outputs:
- grad_input: bfloat16 [8192, 1024], P(('fsdp', 'dp'))
- grad_weight: float32 [1024, 4096], P('fsdp')
- grad_gain: float32 [4096], replicated
- grad_shift: float32 [4096], replicated
The draws below stay inside these ranges and needn't reach their ends.
All inputs are finite; a program needn't handle non-finite values. No bound on the sum of `relu_mask` on one device may be relied on, other than what follows from the above.
Results may differ from the reference program's by a relative error of at most 0.005.
Values may be sent and summed in bfloat16 or wider, within the bound.
No kernel may reach another device: no remote copies, remote signals or barrier semaphores. Data moves between devices by JAX's collectives and lax.ppermute only.
A program may use at most 128 MiB of HBM per device.

```python
import math
import jax
import jax.numpy as jnp
from jax import lax

DIN = 1024
DOUT = 4096
ROWS = 8192


def draw_cotangent(key, part):
    keys = jax.random.split(jax.random.fold_in(key, 11), 3)
    position = jnp.arange(ROWS).astype(jnp.float32) / ROWS
    rising = 3.0 ** position
    column_scale = 10.0 ** jax.random.uniform(keys[1], (DOUT,), jnp.float32)
    row_scale = rising * 10.0 ** (0.5 * jax.random.uniform(keys[0], (ROWS,), jnp.float32))
    noise = jnp.clip(jax.random.normal(keys[2], (ROWS, DOUT), jnp.float32), -4.0, 4.0)
    values = 0.05 * noise * row_scale[:, None] * column_scale[None, :]
    return values.astype(jnp.bfloat16)


def with_ends(values, own_key, low, top_value):
    dims = values.shape
    place = [jax.random.randint(jax.random.fold_in(own_key, axis), (), 0, dims[axis]) for axis in range(len(dims))]
    values = values.at[tuple(place)].set(low)
    longest = dims.index(max(dims))
    place[longest] = (place[longest] + 1) % dims[longest]
    return values.at[tuple(place)].set(top_value)


def with_spikes(drawn, key, source, target, parts, factor):
    owner, partner = [(jnp.arange(drawn.shape[dim]) // (drawn.shape[dim] // parts)).reshape([-1 if axis == dim else 1 for axis in range(drawn.ndim)]) for dim in (source, target)]
    chosen = jax.random.permutation(key, parts)[partner]
    strong = (owner == chosen) | (owner == (partner + parts // 2) % parts)
    return jnp.where(strong, factor * drawn, drawn)


def block_levels(stream_key, dims, cuts, smallest, top_value):
    def one(dim, parts):
        heights = jax.random.uniform(jax.random.fold_in(jax.random.fold_in(stream_key, 6), dim), (parts,), jnp.float32, smallest / len(cuts), top_value / len(cuts))
        return jnp.repeat(jnp.exp(heights), dims[dim] // parts).reshape((-1,) + (1,) * (len(dims) - dim - 1))

    loudness = one(*cuts[0])
    for cut in cuts[1:]:
        loudness = loudness * one(*cut)
    return loudness


def centred(key, shape, width, reach, cuts=(), held_as=jnp.bfloat16):
    factor_of = block_levels(key, shape, cuts, -0.22, 0.18) if cuts else 1.0
    array = jax.random.normal(key, shape, jnp.float32) * width * factor_of
    return jnp.minimum(jnp.maximum(array, -reach), reach).astype(held_as)


def bell_draw_with(stream_key, extent, width, most, cuts, heavy, dtype=jnp.bfloat16):
    result = width * jax.random.normal(stream_key, extent, jnp.float32)
    if cuts:
        result = result * block_levels(stream_key, extent, cuts, -0.22, 0.18)
    return jnp.clip(with_spikes(result, jax.random.fold_in(stream_key, 3), *heavy), -most, most).astype(dtype)


def setup_inputs(seed: int = 0) -> dict:
    key_of = jax.random.split(jax.random.key(seed), 8)
    features = bell_draw_with(key_of[0], (ROWS, DIN), 1.0, 6.0, ((0, 32),), (0, 1, 32, 2.75))
    normed = centred(key_of[1], (ROWS, DOUT), 1.0, 6.0, ((0, 32),))
    relu_mask = with_ends((jax.random.randint(key_of[2], (ROWS, DOUT), 0, 2) < 1).astype(jnp.int32), jax.random.fold_in(key_of[2], 1), 0, 1)
    cotangent = draw_cotangent(jax.random.fold_in(key_of[7], 71), 0)
    weight_shard = centred(key_of[4], (DIN, DOUT), DIN ** -0.5, 0.1875, ((0, 8),))
    norm_gain = jnp.clip(1.0 + 0.15 * jax.random.normal(key_of[5], (DOUT,), jnp.float32), 0.25, 1.75)
    inverse_deviation = jnp.clip(jnp.exp(jax.random.uniform(key_of[6], (DOUT,), jnp.float32, math.log(0.5), math.log(3.0))), 0.5, 3.0)
    return {"features": features, "normed": normed, "relu_mask": relu_mask, "cotangent": cotangent, "weight_shard": weight_shard, "norm_gain": norm_gain, "inverse_deviation": inverse_deviation}


def reference(features, normed, relu_mask, cotangent, weight_shard, norm_gain, inverse_deviation):
    masked = cotangent.astype(jnp.float32) * relu_mask.astype(jnp.float32)
    normed_f = normed.astype(jnp.float32)
    sum_plain = lax.optimization_barrier(jnp.sum(masked, axis=0))
    sum_cross = lax.optimization_barrier(jnp.sum(masked * normed_f, axis=0))
    norm_grad = inverse_deviation * norm_gain * (masked - sum_plain / ROWS - normed_f * (sum_cross / ROWS))
    norm_grad = norm_grad.astype(jnp.bfloat16)
    grad_input = jnp.dot(norm_grad, weight_shard.T, preferred_element_type=jnp.float32).astype(jnp.bfloat16)
    rescale = 1.0 / math.sqrt(ROWS)
    grad_weight = jnp.dot(features.T, norm_grad, preferred_element_type=jnp.float32) * rescale
    return (grad_input, grad_weight, sum_cross * rescale, sum_plain * rescale)
```

```python
import functools
import math

import jax
import jax.numpy as jnp
from jax import lax
from jax.experimental import pallas as pl
from jax.experimental.pallas import tpu as pltpu
from jax.sharding import PartitionSpec as P

F32 = jnp.float32
BF16 = jnp.bfloat16


def swap(x, axis, bit):
    size = lax.axis_size(axis)
    return lax.ppermute(x, axis, [(i, i ^ bit) for i in range(size)])


def bits_of(size):
    return [1 << b for b in range(size.bit_length() - 1)]


def column_blocks(columns):
    width = 512
    while columns % width:
        width //= 2
    return width


def sums_kernel(cot_ref, mask_ref, normed_ref, masked_ref, sums_ref):
    masked = cot_ref[...].astype(F32) * mask_ref[...].astype(F32)
    masked_ref[...] = masked.astype(BF16)
    sums_ref[0:1, :] = jnp.sum(masked, axis=0, keepdims=True)
    sums_ref[1:2, :] = jnp.sum(masked * normed_ref[...].astype(F32), axis=0, keepdims=True)


def local_sums(cotangent, relu_mask, normed):
    rows, units = cotangent.shape
    width = column_blocks(units)
    spec = pl.BlockSpec((rows, width), lambda i: (0, i))
    return pl.pallas_call(
        sums_kernel,
        grid=(units // width,),
        in_specs=[spec, spec, spec],
        out_specs=[spec, pl.BlockSpec((2, width), lambda i: (0, i))],
        out_shape=[
            jax.ShapeDtypeStruct((rows, units), BF16),
            jax.ShapeDtypeStruct((2, units), F32),
        ],
        cost_estimate=pl.CostEstimate(flops=8 * rows * units, bytes_accessed=10 * rows * units, transcendentals=0),
        name="local_sums",
    )(cotangent, relu_mask, normed)


def grad_kernel(total_rows, order_ref, masked_ref, normed_ref, sums_ref, scale_ref, out_ref):
    mean_plain = sums_ref[0:1, :] / total_rows
    mean_cross = sums_ref[1:2, :] / total_rows
    scale = scale_ref[0:1, :] * scale_ref[1:2, :]
    value = scale * (
        masked_ref[...].astype(F32) - mean_plain - normed_ref[...].astype(F32) * mean_cross
    )
    out_ref[0] = value.astype(BF16)


def norm_grad_blocks(order, masked, normed, sums, scales, parts, total_rows):
    rows, units = masked.shape
    width = units // parts
    wide = pl.BlockSpec((rows, width), lambda i, order: (0, order[i]))
    thin = pl.BlockSpec((2, width), lambda i, order: (0, order[i]))
    return pl.pallas_call(
        functools.partial(grad_kernel, total_rows),
        grid_spec=pltpu.PrefetchScalarGridSpec(
            num_scalar_prefetch=1,
            grid=(parts,),
            in_specs=[wide, wide, thin, thin],
            out_specs=pl.BlockSpec((1, rows, width), lambda i, order: (i, 0, 0)),
        ),
        out_shape=jax.ShapeDtypeStruct((parts, rows, width), BF16),
        cost_estimate=pl.CostEstimate(flops=8 * rows * units, bytes_accessed=6 * rows * units, transcendentals=0),
        name="norm_grad",
    )(order, masked, normed, sums, scales)


def place_kernel(rescale, order_ref, part_ref, out_ref):
    out_ref[...] = part_ref[0].astype(F32) * rescale


def place_units(order, pieces, rescale):
    parts, rows, width = pieces.shape
    return pl.pallas_call(
        functools.partial(place_kernel, rescale),
        grid_spec=pltpu.PrefetchScalarGridSpec(
            num_scalar_prefetch=1,
            grid=(parts,),
            in_specs=[pl.BlockSpec((1, rows, width), lambda i, order: (i, 0, 0))],
            out_specs=pl.BlockSpec((rows, width), lambda i, order: (0, order[i])),
        ),
        out_shape=jax.ShapeDtypeStruct((rows, parts * width), F32),
        cost_estimate=pl.CostEstimate(flops=rows * parts * width, bytes_accessed=6 * rows * parts * width, transcendentals=0),
        name="place_units",
    )(order, pieces)


def reversed_bits(values, bits):
    out = values * 0
    for place, bit in enumerate(bits):
        out = out + ((values // bit) % 2) * bits[len(bits) - 1 - place]
    return out


def on_device(features, normed, relu_mask, cotangent, weight_shard, norm_gain, inverse_deviation):
    rows, inputs = features.shape
    units = normed.shape[1]
    fsdp, dp = lax.axis_size("fsdp"), lax.axis_size("dp")
    total_rows = rows * fsdp * dp
    width = units // dp
    f, d = lax.axis_index("fsdp"), lax.axis_index("dp")
    dp_bits, fsdp_bits = bits_of(dp), bits_of(fsdp)
    dp_place = reversed_bits(jnp.arange(dp, dtype=jnp.int32), dp_bits)
    order = jnp.bitwise_xor(d.astype(jnp.int32), dp_place)

    weight = lax.dynamic_slice_in_dim(weight_shard, d * width, width, axis=1)[None]
    for bit in reversed(fsdp_bits):
        weight = jnp.concatenate([weight, swap(weight, "fsdp", bit)], axis=0)
    weight_place = reversed_bits(jnp.bitwise_xor(f, jnp.arange(fsdp, dtype=jnp.int32)), fsdp_bits)
    weight = jnp.take(weight, weight_place, axis=0, mode="clip").reshape(inputs, width)

    group = features[None]
    for bit in reversed(dp_bits):
        group = jnp.concatenate([group, swap(group, "dp", bit)], axis=0)

    masked, own_sums = local_sums(cotangent, relu_mask, normed)
    everyone = ("fsdp", "dp")
    spread = own_sums.reshape(fsdp * dp, -1)
    spread = lax.all_to_all(spread, everyone, split_axis=0, concat_axis=0, tiled=True)
    owned = jnp.sum(spread, axis=0, keepdims=True)
    spread = jnp.broadcast_to(owned, spread.shape)
    spread = lax.all_to_all(spread, everyone, split_axis=0, concat_axis=0, tiled=True)
    sums = spread.reshape(2, units)

    scales = jnp.stack([inverse_deviation, norm_gain])
    blocks = norm_grad_blocks(order, masked, normed, sums, scales, dp, total_rows)

    blocks = blocks.reshape((2,) * len(dp_bits) + (rows, width))
    for axis, bit in reversed(list(enumerate(dp_bits))):
        away = lax.index_in_dim(blocks, 1, axis, keepdims=True)
        here = lax.index_in_dim(blocks, 0, axis, keepdims=True)
        blocks = jnp.concatenate([here, swap(away, "dp", bit)], axis=axis)
    grads = blocks.reshape(dp * rows, width)

    term = lax.dot_general(
        group.reshape(dp * rows, inputs), grads, (((0,), (0,)), ((), ())), preferred_element_type=F32
    ).astype(BF16)
    part = lax.dot_general(
        grads, weight, (((1,), (1,)), ((), ())), preferred_element_type=F32
    ).reshape((2,) * len(dp_bits) + (rows, inputs))

    term = lax.all_to_all(
        term.reshape(fsdp, inputs // fsdp, width), "fsdp", split_axis=0, concat_axis=0, tiled=True
    )
    pieces = jnp.sum(term.astype(F32), axis=0).astype(BF16)[None]
    for bit in reversed(dp_bits):
        pieces = jnp.concatenate([pieces, swap(pieces, "dp", bit)], axis=0)
    rescale = 1.0 / math.sqrt(total_rows)
    grad_weight = place_units(order, pieces, rescale)

    for bit in dp_bits:
        part = part[0] + swap(part[1].astype(BF16), "dp", bit).astype(F32)
    return (part.astype(BF16), grad_weight, sums[1] * rescale, sums[0] * rescale)


def solution(mesh):
    rows = P(("fsdp", "dp"), None)
    return jax.shard_map(
        on_device,
        mesh=mesh,
        in_specs=(rows, rows, rows, rows, P("fsdp", None), P(), P()),
        out_specs=(rows, P("fsdp", None), P(), P()),
        check_vma=False,
    )
```

```python
import functools
import math

import jax
import jax.numpy as jnp
from jax import lax
from jax.experimental import pallas as pl
from jax.experimental.pallas import tpu as pltpu
from jax.sharding import PartitionSpec as P


F32 = jnp.float32
BF16 = jnp.bfloat16


def swap(x, axis, offset):
    size = lax.axis_size(axis)
    return lax.ppermute(x, axis, [(i, i ^ offset) for i in range(size)])


def bits_of(size):
    return [1 << b for b in range(size.bit_length() - 1)]


def offsets(bits):
    found = [0]
    for bit in bits:
        found = found + [offset ^ bit for offset in found]
    return found


def cost(flops, moved):
    return pl.CostEstimate(flops=flops, bytes_accessed=moved, transcendentals=0)


def sums_kernel(cot_ref, mask_ref, normed_ref, masked_ref, sums_ref, total_ref):
    step, last = pl.program_id(0), pl.num_programs(0) - 1
    rows, units = cot_ref.shape
    tiles = units // 128

    @pl.when(step == 0)
    def _():
        total_ref[...] = jnp.zeros_like(total_ref)

    for tile in range(tiles):
        columns = slice(tile * 128, tile * 128 + 128)
        masked = cot_ref[:, columns].astype(F32) * mask_ref[:, columns].astype(F32)
        masked_ref[:, columns] = masked.astype(BF16)
        cross = masked * normed_ref[:, columns].astype(F32)
        total_ref[0, :, columns] += jnp.sum(masked.reshape(rows // 8, 8, 128), axis=0)
        total_ref[1, :, columns] += jnp.sum(cross.reshape(rows // 8, 8, 128), axis=0)

    @pl.when(step == last)
    def _():
        for tile in range(tiles):
            columns = slice(tile * 128, tile * 128 + 128)
            for which in range(2):
                sums_ref[which * tiles + tile] = jnp.sum(
                    total_ref[which, :, columns], axis=0, keepdims=True
                )


def local_sums(cotangent, relu_mask, normed):
    rows, units = cotangent.shape
    depth = 64
    spec = pl.BlockSpec((depth, units), lambda i: (i, 0))
    lines = 2 * units // 128
    return pl.pallas_call(
        sums_kernel,
        grid=(rows // depth,),
        in_specs=[spec, spec, spec],
        out_specs=[spec, pl.BlockSpec((lines, 1, 128), lambda i: (0, 0, 0))],
        out_shape=[
            jax.ShapeDtypeStruct((rows, units), BF16),
            jax.ShapeDtypeStruct((lines, 1, 128), F32),
        ],
        scratch_shapes=[pltpu.VMEM((2, 8, units), F32)],
        cost_estimate=cost(8 * rows * units, 10 * rows * units),
        name="local_sums",
    )(cotangent, relu_mask, normed)


def grad_kernel(total_rows, block_ref, masked_ref, normed_ref, plain_ref, cross_ref, inverse_ref, gain_ref, *outs):
    for at, out_ref in enumerate(outs):

        @pl.when(pl.program_id(0) == at)
        def _():
            for tile in range(out_ref.shape[1] // 128):
                columns = slice(tile * 128, tile * 128 + 128)
                mean_plain = plain_ref[tile] / total_rows
                mean_cross = cross_ref[tile] / total_rows
                scale = inverse_ref[tile] * gain_ref[tile]
                value = scale * (
                    masked_ref[:, columns].astype(F32)
                    - mean_plain
                    - normed_ref[:, columns].astype(F32) * mean_cross
                )
                out_ref[:, columns] = value.astype(BF16)


def norm_grads(blocks, masked, normed, sums, inverse, gain, width, total_rows):
    rows, units = masked.shape
    lines = width // 128
    wide = pl.BlockSpec((rows, width), lambda i, block: (0, block[i]))
    thin = pl.BlockSpec((lines, 1, 128), lambda i, block: (block[i], 0, 0))
    later = pl.BlockSpec((lines, 1, 128), lambda i, block: (units // width + block[i], 0, 0))
    count = len(blocks)
    return pl.pallas_call(
        functools.partial(grad_kernel, total_rows),
        grid_spec=pltpu.PrefetchScalarGridSpec(
            num_scalar_prefetch=1,
            grid=(count,),
            in_specs=[wide, wide, thin, later, thin, thin],
            out_specs=[pl.BlockSpec((rows, width), lambda i, block: (0, 0))] * count,
        ),
        out_shape=[jax.ShapeDtypeStruct((rows, width), BF16)] * count,
        cost_estimate=cost(8 * count * rows * width, 6 * count * rows * width),
        name="norm_grad",
    )(jnp.stack(blocks), masked, normed, sums, sums, inverse, gain)


def term_kernel(parts, order_ref, *refs):
    away_ref, kept_ref = refs[-2:]
    grads = refs[2 * parts : 3 * parts]
    for out_ref, rows in ((away_ref, refs[:parts]), (kept_ref, refs[parts : 2 * parts])):
        total = 0.0
        for row_ref, grad_ref in zip(rows, grads):
            total = total + lax.dot_general(
                row_ref[...], grad_ref[...], (((0,), (0,)), ((), ())), preferred_element_type=F32
            )
        out_ref[0] = total.astype(out_ref.dtype)


def weight_term(order, group, grads, blocks):
    rows, inputs = group[0].shape
    width = grads[0].shape[1]
    deep = inputs // blocks
    half, parts = blocks // 2, len(group)
    if deep % 128:
        total = 0.0
        for row, grad in zip(group, grads):
            total = total + lax.dot_general(
                row, grad, (((0,), (0,)), ((), ())), preferred_element_type=F32
            )
        total = jnp.take(total.reshape(blocks, deep, width), order, axis=0, mode="clip")
        return total[:half].astype(BF16), total[half:]
    away = pl.BlockSpec((rows, deep), lambda i, order: (0, order[i]))
    kept = pl.BlockSpec((rows, deep), lambda i, order: (0, order[half + i]))
    whole = pl.BlockSpec((rows, width), lambda i, order: (0, 0))
    out = pl.BlockSpec((1, deep, width), lambda i, order: (i, 0, 0))
    return pl.pallas_call(
        functools.partial(term_kernel, parts),
        grid_spec=pltpu.PrefetchScalarGridSpec(
            num_scalar_prefetch=1,
            grid=(half,),
            in_specs=[away] * parts + [kept] * parts + [whole] * parts,
            out_specs=[out, out],
        ),
        out_shape=[
            jax.ShapeDtypeStruct((half, deep, width), BF16),
            jax.ShapeDtypeStruct((half, deep, width), F32),
        ],
        cost_estimate=cost(2 * parts * rows * inputs * width, 5 * inputs * width + 4 * parts * rows * inputs),
        name="weight_term",
    )(order, *group, *group, *grads)


def rows_kernel(chunks, steps, order_ref, *refs):
    away_ref, kept_ref = refs[-2:]
    grads = refs[len(steps) : -2]
    parts = len(grads) // chunks
    half = parts // 2
    first = 0
    for weight_ref, count in zip(refs, steps):

        @pl.when(jnp.logical_and(pl.program_id(0) >= first, pl.program_id(0) < first + count))
        def _():
            blocks, deep, units = weight_ref.shape
            weight = weight_ref[...].reshape(blocks * deep, units)
            width = units // chunks
            for part in range(parts):
                total = 0.0
                for chunk in range(chunks):
                    total = total + lax.dot_general(
                        grads[part * chunks + chunk][...],
                        weight[:, chunk * width : (chunk + 1) * width],
                        (((1,), (1,)), ((), ())),
                        preferred_element_type=F32,
                    )
                out_ref = kept_ref if part < half else away_ref
                for block in range(blocks):
                    place = order_ref[pl.program_id(0) * blocks + block]
                    columns = pl.ds(pl.multiple_of(place * deep, deep), deep)
                    out_ref[part % half, :, columns] = total[
                        :, block * deep : (block + 1) * deep
                    ].astype(out_ref.dtype)

        first += count


def input_terms(order, weights, grads):
    parts, chunks = len(grads), len(grads[0])
    rows, width = grads[0][0].shape
    deep, units = weights[0].shape[1:]
    blocks = 2 if deep < 256 else 1
    steps = [weight.shape[0] // blocks for weight in weights]
    specs, first = [], 0
    for count in steps:
        specs.append(
            pl.BlockSpec(
                (blocks, deep, units),
                lambda i, order, first=first, count=count: (jnp.clip(i - first, 0, count - 1), 0, 0),
            )
        )
        first += count
    inputs = order.shape[0] * deep
    flat = [piece for part in grads for piece in part]
    whole = pl.BlockSpec((rows, width), lambda i, order: (0, 0))
    out = pl.BlockSpec((parts // 2, rows, inputs), lambda i, order: (0, 0, 0))
    return pl.pallas_call(
        functools.partial(rows_kernel, chunks, steps),
        grid_spec=pltpu.PrefetchScalarGridSpec(
            num_scalar_prefetch=1,
            grid=(sum(steps),),
            in_specs=specs + [whole] * len(flat),
            out_specs=[out, out],
        ),
        out_shape=[
            jax.ShapeDtypeStruct((parts // 2, rows, inputs), BF16),
            jax.ShapeDtypeStruct((parts // 2, rows, inputs), F32),
        ],
        cost_estimate=cost(2 * parts * rows * inputs * units, 3 * parts * rows * inputs + 2 * inputs * units),
        name="input_terms",
    )(order, *weights, *flat)


def place_kernel(rescale, chunks, order_ref, *refs):
    out_ref = refs[-1]
    parts = (len(refs) - 1) // chunks
    width = out_ref.shape[1] // chunks
    for part in range(parts):

        @pl.when(pl.program_id(0) == part)
        def _():
            for chunk in range(chunks):
                piece = refs[part * chunks + chunk][...]
                out_ref[:, chunk * width : (chunk + 1) * width] = piece.astype(F32) * rescale


def place_units(order, pieces, rescale):
    parts, chunks = len(pieces), len(pieces[0])
    rows, width = pieces[0][0].shape
    flat = [piece for part in pieces for piece in part]
    return pl.pallas_call(
        functools.partial(place_kernel, rescale, chunks),
        grid_spec=pltpu.PrefetchScalarGridSpec(
            num_scalar_prefetch=1,
            grid=(parts,),
            in_specs=[pl.BlockSpec((rows, width), lambda i, order: (0, 0))] * len(flat),
            out_specs=pl.BlockSpec((rows, chunks * width), lambda i, order: (0, order[i])),
        ),
        out_shape=jax.ShapeDtypeStruct((rows, parts * chunks * width), F32),
        cost_estimate=cost(rows * parts * chunks * width, 6 * rows * parts * chunks * width),
        name="place_units",
    )(order, *flat)


def everyones_sum(own):
    everyone = ("fsdp", "dp")
    parts = lax.axis_size("fsdp") * lax.axis_size("dp")
    lines = own.shape[0]
    spread = own if lines % parts == 0 else own.reshape(parts, 1, -1)
    size = spread.shape[0] // parts
    spread = lax.all_to_all(spread, everyone, split_axis=0, concat_axis=0, tiled=True)
    owned = jnp.sum(spread.reshape(parts, size, 1, -1), axis=0, keepdims=True)
    spread = jnp.broadcast_to(owned, (parts,) + owned.shape[1:]).reshape(spread.shape)
    spread = lax.all_to_all(spread, everyone, split_axis=0, concat_axis=0, tiled=True)
    return spread.reshape(own.shape)


def chunks_of(width):
    return 2 if width % 256 == 0 else 1


def on_device(features, normed, relu_mask, cotangent, weight_shard, norm_gain, inverse_deviation):
    rows, inputs = features.shape
    units = normed.shape[1]
    fsdp, dp = lax.axis_size("fsdp"), lax.axis_size("dp")
    total_rows = rows * fsdp * dp
    width = units // dp
    chunks = chunks_of(width)
    part_width = width // chunks
    f, d = lax.axis_index("fsdp"), lax.axis_index("dp")
    f, d = f.astype(jnp.int32), d.astype(jnp.int32)
    dp_bits, fsdp_bits = bits_of(dp), bits_of(fsdp)
    partners = list(range(dp))
    deep = inputs // fsdp

    weight_bits = fsdp_bits[-1:] + fsdp_bits[:-1]
    weight = lax.dynamic_slice_in_dim(weight_shard, d * width, width, axis=1)[None]
    for at, bit in enumerate(weight_bits):
        came = swap(weight, "fsdp", bit)
        if at < len(weight_bits) - 1:
            weight = jnp.concatenate([weight, came], axis=0)
    input_order = jnp.bitwise_xor(f, jnp.array(offsets(weight_bits), jnp.int32))
    weights = [weight, came]
    if deep % 128:
        weight = jnp.concatenate(weights, axis=0)
        back = jnp.zeros_like(input_order).at[input_order].set(jnp.arange(fsdp, dtype=jnp.int32))
        weights = [jnp.take(weight, back, axis=0, mode="clip").reshape(inputs // 128, 128, width)]
        input_order = jnp.arange(inputs // 128, dtype=jnp.int32)

    group = {0: features}
    for bit in reversed(dp_bits):
        for k in list(group):
            group[k ^ bit] = swap(group[k], "dp", bit)

    masked, own_sums = local_sums(cotangent, relu_mask, normed)
    sums = everyones_sum(own_sums)
    lined = lambda vector: vector.reshape(-1, 1, 128)

    grads = [{} for _ in range(chunks)]
    near = [k for k in partners if k < dp // 2]
    far = [k for k in reversed(partners) if k >= dp // 2]
    turns = [[(chunk, k) for k in far] for chunk in range(chunks)]
    turns.append([(chunk, k) for chunk in range(chunks) for k in reversed(near)])
    for turn in turns:
        blocks = [jnp.bitwise_xor(d, k) * chunks + chunk for chunk, k in turn]
        pieces = norm_grads(
            blocks, masked, normed, sums, lined(inverse_deviation), lined(norm_gain),
            part_width, total_rows,
        )
        for (chunk, k), piece in zip(turn, pieces):
            grads[chunk][k] = swap(piece, "dp", k) if k else piece

    places = offsets(list(reversed(fsdp_bits)))
    term_order = jnp.bitwise_xor(f, jnp.array(places[fsdp // 2 :] + places[: fsdp // 2], jnp.int32))
    finished = []
    for chunk in range(chunks):
        away, kept = weight_term(
            term_order, [group[k] for k in partners],
            [grads[chunk][k] for k in partners], fsdp,
        )
        for bit in fsdp_bits:
            came = swap(away, "fsdp", bit)
            half = kept.shape[0] // 2
            if half:
                away = (kept[half:] + came[half:].astype(F32)).astype(BF16)
                kept = kept[:half] + came[:half].astype(F32)
            else:
                kept = kept + came.astype(F32)
        pieces = {0: kept.reshape(deep, part_width).astype(BF16)}
        for bit in reversed(dp_bits):
            for k in list(pieces):
                pieces[k ^ bit] = swap(pieces[k], "dp", bit)
        finished.append(pieces)
    rescale = 1.0 / math.sqrt(total_rows)
    unit_order = jnp.bitwise_xor(d, jnp.arange(dp, dtype=jnp.int32))
    grad_weight = place_units(
        unit_order, [[finished[c][k] for c in range(chunks)] for k in partners], rescale
    )

    places = offsets(list(reversed(dp_bits)))
    away, kept = input_terms(
        input_order, weights, [[grads[c][k] for c in range(chunks)] for k in places]
    )
    for bit in dp_bits:
        came = swap(away, "dp", bit)
        half = kept.shape[0] // 2
        if half:
            away = (kept[half:] + came[half:].astype(F32)).astype(BF16)
            kept = kept[:half] + came[:half].astype(F32)
        else:
            kept = kept + came.astype(F32)
    sums = sums.reshape(2, units) * rescale
    return (kept.reshape(rows, inputs).astype(BF16), grad_weight, sums[1], sums[0])


def solution(mesh):
    rows = P(("fsdp", "dp"), None)
    return jax.shard_map(
        on_device,
        mesh=mesh,
        in_specs=(rows, rows, rows, rows, P("fsdp", None), P(), P()),
        out_specs=(rows, P("fsdp", None), P(), P()),
        check_vma=False,
    )
```
